32 devices in a mesh: tm: 4 (over y, x), space: 8 (over z, core).
Axes of the slice: x: 2, y: 2, z: 4, core: 2. Of those that a mesh axis runs over, the one named last changes fastest.
Arguments:
- residual_field: float32 [64, 128, 128, 128], P('tm', 'space'), may hold values from -6 to 6
- eigvec_x: float32 [128, 128], replicated, may hold values from -1 to 1, as said below
- eigvec_y: float32 [128, 128], replicated, may hold values from -1 to 1, as said below
- eigvec_z: float32 [128, 128], replicated, may hold values from -1 to 1, as said below
- eigval_x: float32 [128], replicated, may hold values from 0.0001 to 0.05
- eigval_y: float32 [128], replicated, may hold values from 0.0001 to 0.05
- eigval_z: float32 [128], replicated, may hold values from 0.0001 to 0.05
Outputs:
- update: float32 [64, 128, 128, 128], P('tm', 'space')
The draws below stay inside these ranges and needn't reach their ends.
Inputs may be any that keep to these rules, and one draw needn't show every extreme that they name: `eigvec_x`: an orthogonal matrix. `eigvec_y`: an orthogonal matrix. `eigvec_z`: an orthogonal matrix.
All inputs are finite; a program needn't handle non-finite values.
Results may differ from the reference program's by a relative error of at most 0.00025.
Values sent between devices are 32-bit elements; how exact they have to be, the bound alone decides.
No kernel may reach another device: no remote copies, remote signals or barrier semaphores. Data moves between devices by JAX's collectives and lax.ppermute only.
A program may use at most 256 MiB of HBM per device.

```python
import math
import jax
import jax.numpy as jnp
from jax import lax

L = 64
NX = 128
NY = 128
NZ = 128


def orthogonal(key, dimension):

    def reflect(source, matrix):
        vector = jax.random.normal(jax.random.fold_in(key, source), (dimension,), jnp.float32)
        vector = vector / jnp.sqrt(jnp.sum(vector * vector))
        return matrix - 2.0 * jnp.outer(jnp.dot(matrix, vector), vector)
    return lax.fori_loop(0, dimension, reflect, jnp.eye(dimension, dtype=jnp.float32))


def draw_eigvec_x(key, part):
    return orthogonal(jax.random.fold_in(key, 101), NX)


def draw_eigvec_y(key, part):
    return orthogonal(jax.random.fold_in(key, 202), NY)


def draw_eigvec_z(key, part):
    return orthogonal(jax.random.fold_in(key, 303), NZ)


def shard_levels(own_key, dims, cuts, low, top_value):
    gain, own = 1.0, jax.random.fold_in(own_key, 6)
    for position, parts in cuts:
        steps = jnp.exp(jax.random.uniform(jax.random.fold_in(own, position), (parts,), jnp.float32, low / len(cuts), top_value / len(cuts)))
        gain = gain * jnp.repeat(steps, dims[position] // parts).reshape([-1 if axis == position else 1 for axis in range(len(dims))])
    return gain


def gaussian(key, shape, spread, most, pieces=(), held_as=jnp.bfloat16):
    loudness = shard_levels(key, shape, pieces, -0.22, 0.18) if pieces else 1.0
    values = jax.random.normal(key, shape, jnp.float32) * spread * loudness
    return jnp.minimum(jnp.maximum(values, -most), most).astype(held_as)


def setup_inputs(seed: int = 0) -> dict:
    arg_keys = jax.random.split(jax.random.key(seed), 8)
    return {
        "residual_field": gaussian(arg_keys[0], (L, NX, NY, NZ), 1.0, 6.0, ((0, 4), (1, 8)), jnp.float32),
        "eigvec_x": draw_eigvec_x(jax.random.fold_in(arg_keys[7], 71), 0),
        "eigvec_y": draw_eigvec_y(jax.random.fold_in(arg_keys[7], 71), 0),
        "eigvec_z": draw_eigvec_z(jax.random.fold_in(arg_keys[7], 71), 0),
        "eigval_x": jnp.clip(jnp.exp(jax.random.uniform(arg_keys[4], (NX,), jnp.float32, math.log(0.0001), math.log(0.05))), 0.0001, 0.05),
        "eigval_y": jnp.clip(jnp.exp(jax.random.uniform(arg_keys[5], (NY,), jnp.float32, math.log(0.0001), math.log(0.05))), 0.0001, 0.05),
        "eigval_z": jnp.clip(jnp.exp(jax.random.uniform(arg_keys[6], (NZ,), jnp.float32, math.log(0.0001), math.log(0.05))), 0.0001, 0.05),
    }


highest = lax.Precision.HIGHEST
circulant_alpha = 0.01


def spectral_solve(values, shifts, total_steps):
    step_ids = jnp.arange(total_steps, dtype=jnp.int32)
    phases = (step_ids[:, None] * step_ids[None, :]) % total_steps
    angles = (2.0 * math.pi / total_steps) * phases.astype(jnp.float32)
    cosine = jnp.cos(angles)
    sine_table = jnp.sin(angles)
    root_alpha = circulant_alpha ** (1.0 / total_steps)
    powers = root_alpha ** step_ids.astype(jnp.float32)
    flattened = values.reshape(total_steps, -1) * powers[:, None]
    real_part = jnp.dot(cosine, flattened, precision=highest)
    imag_part = -jnp.dot(sine_table, flattened, precision=highest)
    flat_shift = shifts.reshape(1, -1)
    denom_real = 1.0 + flat_shift - root_alpha * cosine[:, 1:2]
    denom_imag = root_alpha * sine_table[:, 1:2]
    modulus = denom_real * denom_real + denom_imag * denom_imag
    quot_real = (real_part * denom_real + imag_part * denom_imag) / modulus
    quot_imag = (imag_part * denom_real - real_part * denom_imag) / modulus
    restored = jnp.dot(cosine, quot_real, precision=highest) - jnp.dot(sine_table, quot_imag, precision=highest)
    restored = restored / (total_steps * powers[:, None])
    return restored.reshape(values.shape)


def reference(residual_field, eigvec_x, eigvec_y, eigvec_z, eigval_x, eigval_y, eigval_z):
    total_steps = residual_field.shape[0]

    def forward_plane(plane):
        plane = jnp.einsum('xyz,zk->xyk', plane, eigvec_z, precision=highest)
        plane = jnp.einsum('xyk,yj->xjk', plane, eigvec_y, precision=highest)
        return jnp.einsum('xjk,xi->ijk', plane, eigvec_x, precision=highest)

    def inverse_plane(plane):
        plane = jnp.einsum('ijk,zk->ijz', plane, eigvec_z, precision=highest)
        plane = jnp.einsum('ijz,yj->iyz', plane, eigvec_y, precision=highest)
        return jnp.einsum('iyz,xi->xyz', plane, eigvec_x, precision=highest)

    coeffs = lax.map(forward_plane, residual_field)
    shift_yz = eigval_y[:, None] + eigval_z[None, :]

    def solve_slab(source):
        slab = lax.dynamic_index_in_dim(coeffs, source, 1, keepdims=False)
        shift_x = lax.dynamic_index_in_dim(eigval_x, source, 0, keepdims=False)
        return spectral_solve(slab, shift_x + shift_yz, total_steps)

    solved = lax.map(solve_slab, jnp.arange(eigval_x.shape[0], dtype=jnp.int32))
    solved = jnp.moveaxis(solved, 0, 1)
    return lax.map(inverse_plane, solved)
```

```python
import functools

import jax
import jax.numpy as jnp
from jax import lax
from jax.experimental import pallas as pl
from jax.experimental.pallas import tpu as pltpu
from jax.sharding import PartitionSpec as P

circulant_alpha = 0.01
bf16 = jnp.bfloat16
f32 = jnp.float32


def split(value):
    high = value.astype(bf16)
    low = (value - high.astype(f32)).astype(bf16)
    return high, low


def left_weights(matrix):
    high, low = split(matrix)
    upper = jnp.concatenate([high, high], axis=1)
    lower = jnp.concatenate([low, jnp.zeros_like(low)], axis=1)
    return jnp.concatenate([upper, lower], axis=0)


def right_weights(matrix):
    high, low = split(matrix)
    upper = jnp.concatenate([high, low], axis=1)
    lower = jnp.concatenate([high, jnp.zeros_like(low)], axis=1)
    return jnp.concatenate([upper, lower], axis=0)


def from_left(weights, value):
    high, low = split(value)
    both = jnp.dot(weights, jnp.concatenate([high, low], axis=0), preferred_element_type=f32)
    rows = both.shape[0] // 2
    return both[:rows] + both[rows:]


def from_right(value, weights):
    high, low = split(value)
    both = jnp.dot(jnp.concatenate([high, low], axis=1), weights, preferred_element_type=f32)
    columns = both.shape[1] // 2
    return both[:, :columns] + both[:, columns:]


def lanes(first, second):
    return jnp.concatenate([first, second], axis=1)


def forward_kernel(sizes, places, field_ref, wy_ref, *rest):
    outs, (weights, lines) = rest[:-2], rest[-2:]
    rows_x, modes = field_ref.shape[1], wy_ref.shape[0]

    @pl.when(pl.program_id(0) == 0)
    def _():
        weights[...] = left_weights(wy_ref[...])

    for x in range(0, rows_x, 2):
        value = from_left(weights[...], lanes(field_ref[0, x], field_ref[0, x + 1]))
        half = value.shape[1] // 2
        lines[x * modes : (x + 1) * modes] = value[:, :half]
        lines[(x + 1) * modes : (x + 2) * modes] = value[:, half:]
    row, index = 0, 0
    for size in sizes:
        for _ in range(places):
            for j in range(size):
                outs[index][0, j] = lines[pl.ds(row, rows_x, stride=modes), :]
                row += 1
            index += 1


def gather_rows(refs, step, scratch):
    rows = refs[0].shape[2]
    if rows % 8 == 0:
        return jnp.concatenate([ref[step, 0] for ref in refs], axis=0)
    for index, ref in enumerate(refs):
        scratch[index * rows : (index + 1) * rows] = ref[step, 0]
    return scratch[...]


def damping_of(shift_y_ref, shift_xz_ref, start):
    shift = shift_xz_ref[...] + shift_y_ref[start + pl.program_id(0)]
    return 1.0 / (1.0 + shift)


def mode_kernel(places, start, shift_y_ref, shift_xz_ref, wx_ref, wz_ref, *rest):
    blocks = rest[:places]
    partial_ref, final_ref, x_weights, z_weights, damping, rows_0, rows_1 = rest[places:]
    steps = partial_ref.shape[0]

    @pl.when(pl.program_id(0) == 0)
    def _():
        x_weights[...] = left_weights(wx_ref[...])
        z_weights[...] = right_weights(wz_ref[...])

    damping[...] = damping_of(shift_y_ref, shift_xz_ref, start)
    final_ref[0] = jnp.zeros(final_ref.shape[1:], f32)

    def pair(index, carry):
        step = index * 2
        value = lanes(gather_rows(blocks, step, rows_0), gather_rows(blocks, step + 1, rows_1))
        value = from_left(x_weights[...], value)
        half = value.shape[1] // 2
        value = jnp.concatenate([value[:, :half], value[:, half:]], axis=0)
        value = from_right(value, z_weights[...])
        count = value.shape[0] // 2
        decay = damping[...]
        running = decay * (final_ref[0] + value[:count])
        partial_ref[step, 0] = running
        running = decay * (running + value[count:])
        partial_ref[step + 1, 0] = running
        final_ref[0] = running
        return carry

    lax.fori_loop(0, steps // 2, pair, 0)


def solve_kernel(
    places, groups, start, shift_y_ref, factor_ref, shift_xz_ref, wx_ref, wz_ref, partial_ref, *rest
):
    finals = rest[:groups]
    outs = rest[groups : groups + places]
    x_weights, z_weights, damping, entering = rest[groups + places :]
    steps = partial_ref.shape[0]

    @pl.when(pl.program_id(0) == 0)
    def _():
        x_weights[...] = left_weights(wx_ref[...])
        z_weights[...] = right_weights(wz_ref[...])

    decay = damping_of(shift_y_ref, shift_xz_ref, start)
    damping[...] = decay
    block = decay
    power = 1
    while power * 2 <= steps:
        block = block * block
        power *= 2
    for _ in range(steps - power):
        block = block * decay
    total = factor_ref[groups - 1] * finals[groups - 1][0]
    cycle = block
    for index in reversed(range(groups - 1)):
        total = total * block + factor_ref[index] * finals[index][0]
        cycle = cycle * block
    entering[...] = total / (1.0 - circulant_alpha * cycle)

    def pair(index, carry):
        step = index * 2
        decay = damping[...]
        first = decay * entering[...]
        second = decay * first
        entering[...] = second
        value = jnp.concatenate([partial_ref[step, 0] + first, partial_ref[step + 1, 0] + second], axis=0)
        value = from_right(value, z_weights[...])
        count = value.shape[0] // 2
        value = from_left(x_weights[...], lanes(value[:count], value[count:]))
        half = value.shape[1] // 2
        rows = outs[0].shape[2]
        for place in range(places):
            outs[place][step, 0] = value[place * rows : (place + 1) * rows, :half]
            outs[place][step + 1, 0] = value[place * rows : (place + 1) * rows, half:]
        return carry

    lax.fori_loop(0, steps // 2, pair, 0)


def inverse_kernel(sizes, places, has_sum, wy_ref, *rest):
    count = len(sizes) * places
    blocks = rest[:count]
    sum_ref = rest[count] if has_sum else None
    out_ref, weights, lines = rest[-3:]
    rows_x, modes = out_ref.shape[1], wy_ref.shape[1]

    @pl.when(pl.program_id(0) == 0)
    def _():
        weights[...] = left_weights(wy_ref[...])

    row, index = 0, 0
    for size in sizes:
        for _ in range(places):
            for j in range(size):
                lines[pl.ds(row, rows_x, stride=modes), :] = blocks[index][0, j]
                row += 1
            index += 1
    for x in range(0, rows_x, 2):
        value = lanes(lines[x * modes : (x + 1) * modes], lines[(x + 1) * modes : (x + 2) * modes])
        value = from_left(weights[...], value)
        half = value.shape[1] // 2
        first, second = value[:, :half], value[:, half:]
        if has_sum:
            first, second = first + sum_ref[0, x], second + sum_ref[0, x + 1]
        out_ref[0, x] = first
        out_ref[0, x + 1] = second


def whole(shape):
    return pl.BlockSpec(shape, lambda *_: (0,) * len(shape))


def step_block(shape):
    return pl.BlockSpec((1,) + tuple(shape[1:]), lambda t: (t,) + (0,) * (len(shape) - 1))


def mode_block(shape):
    return pl.BlockSpec((shape[0], 1) + tuple(shape[2:]), lambda j: (0, j) + (0,) * (len(shape) - 2))


scalars = pl.BlockSpec(memory_space=pltpu.SMEM)


def cost(planes, size, touched):
    return pl.CostEstimate(flops=6 * planes * size**3, bytes_accessed=touched, transcendentals=0)


def forward(field, weights, sizes, places):
    steps, rows_x, size_y, size_z = field.shape
    shapes = [(steps, size, rows_x, size_z) for size in sizes for _ in range(places)]
    modes = weights.shape[0]
    return pl.pallas_call(
        functools.partial(forward_kernel, sizes, places),
        grid=(steps,),
        in_specs=[step_block(field.shape), whole(weights.shape)],
        out_specs=[step_block(shape) for shape in shapes],
        out_shape=[jax.ShapeDtypeStruct(shape, f32) for shape in shapes],
        scratch_shapes=[
            pltpu.VMEM((2 * modes, 2 * size_y), bf16),
            pltpu.VMEM((rows_x * modes, size_z), f32),
        ],
        cost_estimate=cost(steps * rows_x, size_y, 8 * field.size),
    )(field, weights)


def modes_of(blocks, start, shift_y, shift_xz, wx, wz):
    steps, size, rows_x, size_z = blocks[0].shape
    size_x = wx.shape[0]
    places = len(blocks)
    partial = (steps, size, size_x, size_z)
    final = (size, size_x, size_z)
    return pl.pallas_call(
        functools.partial(mode_kernel, places, start),
        grid=(size,),
        in_specs=[scalars, whole(shift_xz.shape), whole(wx.shape), whole(wz.shape)]
        + [mode_block(blocks[0].shape)] * places,
        out_specs=[mode_block(partial), step_block(final)],
        out_shape=[jax.ShapeDtypeStruct(partial, f32), jax.ShapeDtypeStruct(final, f32)],
        scratch_shapes=[
            pltpu.VMEM((2 * size_x, 2 * size_x), bf16),
            pltpu.VMEM((2 * size_z, 2 * size_z), bf16),
            pltpu.VMEM((size_x, size_z), f32),
            pltpu.VMEM((size_x, size_z), f32),
            pltpu.VMEM((size_x, size_z), f32),
        ],
        cost_estimate=cost(2 * steps * size, size_z, 8 * steps * size * size_x * size_z),
    )(shift_y, shift_xz, wx, wz, *blocks)


def solve(partial, finals, start, shift_y, factors, shift_xz, wx, wz, places):
    steps, size, size_x, size_z = partial.shape
    shape = (steps, size, size_x // places, size_z)
    return pl.pallas_call(
        functools.partial(solve_kernel, places, len(finals), start),
        grid=(size,),
        in_specs=[scalars, scalars, whole(shift_xz.shape), whole(wx.shape), whole(wz.shape)]
        + [mode_block(partial.shape)]
        + [step_block(finals[0].shape)] * len(finals),
        out_specs=[mode_block(shape)] * places,
        out_shape=[jax.ShapeDtypeStruct(shape, f32)] * places,
        scratch_shapes=[
            pltpu.VMEM((2 * size_x, 2 * size_x), bf16),
            pltpu.VMEM((2 * size_z, 2 * size_z), bf16),
            pltpu.VMEM((size_x, size_z), f32),
            pltpu.VMEM((size_x, size_z), f32),
        ],
        cost_estimate=cost(2 * steps * size, size_z, 8 * steps * size * size_x * size_z),
    )(shift_y, factors, shift_xz, wx, wz, partial, *finals)


def inverse(blocks, sizes, weights, sum_so_far, places):
    steps, _, rows_x, size_z = blocks[0].shape
    size_y, modes = weights.shape
    shape = (steps, rows_x, size_y, size_z)
    has_sum = sum_so_far is not None
    operands = [weights, *blocks] + ([sum_so_far] if has_sum else [])
    return pl.pallas_call(
        functools.partial(inverse_kernel, sizes, places, has_sum),
        grid=(steps,),
        in_specs=[whole(weights.shape)]
        + [step_block(block.shape) for block in blocks]
        + ([step_block(shape)] if has_sum else []),
        out_specs=step_block(shape),
        out_shape=jax.ShapeDtypeStruct(shape, f32),
        scratch_shapes=[
            pltpu.VMEM((2 * size_y, 2 * modes), bf16),
            pltpu.VMEM((rows_x * modes, size_z), f32),
        ],
        input_output_aliases={len(operands) - 1: 0} if has_sum else {},
        cost_estimate=cost(steps * rows_x, size_y, 8 * steps * rows_x * size_y * size_z),
    )(*operands)


def exchange(blocks):
    places = len(blocks)
    return [blocks[0]] + [
        lax.ppermute(blocks[k], "space", [(i, i ^ k) for i in range(places)]) for k in range(1, places)
    ]


def chunks(count):
    small = max(1, count // 8)
    sizes = [small]
    while sum(sizes) + small < count:
        sizes.append(min(2 * small, count - small - sum(sizes)))
    return sizes + [count - sum(sizes)]


def shards(residual_field, eigvec_x, eigvec_y, eigvec_z, eigval_x, eigval_y, eigval_z):
    size_y, size_z = residual_field.shape[2:]
    places = lax.axis_size("space")
    groups = lax.axis_size("tm")
    place = lax.axis_index("space")
    group = lax.axis_index("tm")
    band = size_y // places
    sizes = chunks(band)
    starts = [sum(sizes[:c]) for c in range(len(sizes))]

    order = place ^ jnp.arange(places, dtype=jnp.int32)
    rows_x = jnp.take(eigvec_x.reshape(places, -1, eigvec_x.shape[1]), order, axis=0)
    rows_x = rows_x.reshape(eigvec_x.shape)
    columns_x = rows_x.T
    bands_y = jnp.take(eigvec_y.T.reshape(places, band, size_y), order, axis=0)
    weights_y = [bands_y[:, s : s + n].reshape(-1, size_y) for s, n in zip(starts, sizes)]
    rest_y = jnp.concatenate(weights_y[1:], axis=0)
    early_y = jnp.concatenate(weights_y[:-1], axis=0).T
    transposed_z = eigvec_z.T
    shift_y = lax.dynamic_slice_in_dim(eigval_y, place * band, band, 0)
    shift_xz = eigval_x[:, None] + eigval_z[None, :]
    factors = jnp.where(jnp.arange(1, groups + 1) > group, circulant_alpha, 1.0).astype(f32)

    sent = [forward(residual_field, weights_y[0], sizes[:1], places)]
    rest = forward(residual_field, rest_y, sizes[1:], places)
    sent += [rest[c * places : (c + 1) * places] for c in range(len(sizes) - 1)]
    returned = []
    for c, start in enumerate(starts):
        blocks = exchange(sent[c])
        partial, final = modes_of(blocks, start, shift_y, shift_xz, columns_x, eigvec_z)
        finals = [
            lax.ppermute(final, "tm", [(i, (i + q) % groups) for i in range(groups)])
            for q in range(1, groups)
        ] + [final]
        back = solve(partial, finals, start, shift_y, factors, shift_xz, rows_x, transposed_z, places)
        returned.append(exchange(back))
    early = [block for blocks in returned[:-1] for block in blocks]
    so_far = inverse(early, sizes[:-1], early_y, None, places)
    return inverse(returned[-1], sizes[-1:], weights_y[-1].T, so_far, places)


def solution(mesh):
    placed = (P("tm", "space", None, None), P(), P(), P(), P(), P(), P())
    return jax.shard_map(
        shards, mesh=mesh, in_specs=placed, out_specs=P("tm", "space", None, None), check_vma=False
    )
```
